32 devices in a mesh: rep: 2 (over core), ep: 16 (over z, y, x).
Axes of the slice: x: 2, y: 2, z: 4, core: 2. Of those that a mesh axis runs over, the one named last changes fastest.
Arguments:
- tokens: bfloat16 [4096, 2048], P(('rep', 'ep')), may hold values from -6 to 6
- gates: float32 [4096], P(('rep', 'ep')), may hold values from 0.25 to 1
- expert_ids: int32 [4096, 1], P(('rep', 'ep')), may hold values from 0 to 3; in each aligned block of 128 rows (0 to 127, 128 to 255, ...) at most 40 rows name the same one
- weight_in: bfloat16 [2048, 16384], P(None, 'ep'), may hold values from -0.125 to 0.125
- weight_out: bfloat16 [16384, 2048], P('ep'), may hold values from -0.09375 to 0.09375
Outputs:
- mixed: bfloat16 [4096, 2048], P(('rep', 'ep'))
The draws below stay inside these ranges and needn't reach their ends.
Inputs may be any that keep to these rules, and one draw needn't show every extreme that they name: `expert_ids`: among the 128 rows of one device no expert is named by more than 40 rows, and some expert is named by exactly that many in some devices' rows; every expert is named somewhere.
All inputs are finite; a program needn't handle non-finite values.
Results may differ from the reference program's by a relative error of at most 0.0057.
Values may be sent and summed in bfloat16 or wider, within the bound.
A program may use at most 64 MiB of HBM per device.

```python
import math
import jax
import jax.numpy as jnp
import numpy as np
from jax import lax

D = 2048
FF_DEV = 1024
SLICES = 4
FFW = 4096
EXPERTS = 4
TOK_DEV = 128
CAP = 24
OCAP = 16
TOKENS = 4096
DEVICES = 32


def block_scale(key, extent, cuts, smallest, largest):
    factor_of = 1.0
    for position, shards_of in cuts:
        steps = jax.random.uniform(jax.random.fold_in(jax.random.fold_in(key, 6), position), (shards_of,), jnp.float32, smallest / len(cuts), largest / len(cuts))
        factor_of = factor_of * jnp.repeat(jnp.exp(steps), extent[position] // shards_of).reshape((-1,) + (1,) * (len(extent) - 1 - position))
    return factor_of


def assign_block(stream_key, own, number, rows, count, top, bound, slope):
    order = jax.random.permutation(stream_key, count)
    packed, ordinary = portions_of(count, rows * top, bound, slope, True), portions_of(count, rows * top, bound, slope, False)
    places = jnp.arange(count)

    def named(lengths, rotation):
        used = int((lengths > 0).sum())
        fixed = max(1, used // 4)
        shifted = fixed + (places - fixed + rotation * (used - fixed)) % max(1, count - fixed)
        return jnp.zeros((count,), jnp.int32).at[order[jnp.where(places < fixed, places, shifted)]].set(jnp.asarray(lengths, jnp.int32))

    lengths = jnp.where(number % 4 == 0, named(packed, number // 4), named(ordinary, number - number // 4 - 1))
    mixed = jax.random.permutation(jax.random.fold_in(own, 3), count)
    source_of, receiver = mixed[0:count // 2 * 2:2], mixed[1:count // 2 * 2:2]
    slack = jnp.minimum(lengths[source_of] - 1, bound - lengths[receiver]) // 2
    slack = jnp.where((source_of == order[0]) | (receiver == order[0]) | (lengths[receiver] == 0), 0, jnp.maximum(slack, 0))
    shifted = jax.random.randint(jax.random.fold_in(own, 4), (count // 2,), 0, 1 << 20) % (slack + 1)
    lengths = lengths.at[source_of].add(-shifted).at[receiver].add(shifted)
    members = jnp.searchsorted(jnp.cumsum(lengths), jnp.arange(rows * top), side="right").astype(jnp.int32)
    grid = members.reshape(top, rows).T
    grid = grid[jax.random.permutation(jax.random.fold_in(own, 1), rows)]
    rotation = jax.random.randint(jax.random.fold_in(own, 2), (rows, 1), 0, top)
    return jnp.take_along_axis(grid, (jnp.arange(top)[None, :] + rotation) % top, axis=1)


def portions_of(number_of, total, reach, lean, full):
    portions = [(1 << 20) // math.isqrt(standing ** lean) + 1 for standing in range(1, number_of + 1)]
    largest = reach if full else min(reach, max(-(-total // number_of), total * portions[0] // sum(portions)))
    least = 1 if total - largest >= number_of - 1 else 0
    holding, spare = [largest] + [least] * (number_of - 1), total - largest - least * (number_of - 1)
    while spare > 0:
        free = [i for i in range(1, number_of) if holding[i] < largest] or [i for i in range(1, number_of) if holding[i] < reach]
        whole, left = sum([portions[i] for i in free]), spare
        for i in free:
            extra = min(reach - holding[i], max(1, left * portions[i] // whole), spare)
            holding[i] = holding[i] + extra
            spare = spare - extra
    return np.array(holding)


def gaussian(stream_key, extent, deviation, reach, shards=(), kind=jnp.bfloat16):
    level = block_scale(stream_key, extent, shards, -0.22, 0.18) if shards else 1.0
    values = jax.random.normal(stream_key, extent, jnp.float32) * deviation * level
    return jnp.minimum(jnp.maximum(values, -reach), reach).astype(kind)


def setup_inputs(seed: int = 0) -> dict:
    splits = jax.random.split(jax.random.key(seed), 6)
    tokens = gaussian(splits[0], (TOKENS, D), 1.0, 6.0, ((0, 32),))
    gates = jnp.clip(jnp.exp(math.log(1.0) - 1.3862944 * jax.random.uniform(splits[1], (TOKENS,), jnp.float32) ** block_scale(splits[1], (TOKENS,), ((0, 32),), -0.2, 0.2)), 0.25, 1.0)
    expert_ids_keys = jax.random.split(jax.random.fold_in(splits[2], 1), TOKENS // TOK_DEV)
    expert_ids_turns = jax.random.permutation(jax.random.fold_in(splits[2], 3), TOKENS // TOK_DEV)
    expert_ids = jax.vmap(lambda own, number: assign_block(jax.random.fold_in(splits[2], 2), own, number, TOK_DEV, EXPERTS, 1, CAP + OCAP, 2))(expert_ids_keys, expert_ids_turns).reshape((TOKENS, 1))
    weight_in = gaussian(splits[3], (D, EXPERTS * FFW), D ** -0.5, 0.125, ((1, 16),))
    weight_out = gaussian(splits[4], (EXPERTS * FFW, D), FFW ** -0.5, 0.09375, ((0, 16),))
    return {"tokens": tokens, "gates": gates, "expert_ids": expert_ids, "weight_in": weight_in, "weight_out": weight_out}


def reference(tokens, gates, expert_ids, weight_in, weight_out):
    expert_of = expert_ids[:, 0]
    total_rows = tokens.shape[0]
    width = tokens.shape[1]
    block_rows = DEVICES * (CAP + OCAP)
    order = jnp.argsort(expert_of, stable=True).astype(jnp.int32)
    ordered = tokens[order]
    padded = jnp.concatenate([ordered, jnp.zeros((block_rows, width), ordered.dtype)], axis=0)
    counts = jnp.sum((expert_of[:, None] == jnp.arange(EXPERTS, dtype=jnp.int32)[None, :]).astype(jnp.int32), axis=0)
    starts = (jnp.cumsum(counts) - counts).astype(jnp.int32)

    def serve(results, expert):
        start = starts[expert]
        block = lax.dynamic_slice_in_dim(padded, start, block_rows, 0)
        first = lax.dynamic_slice_in_dim(weight_in, expert * FFW, FFW, 1)
        second = lax.dynamic_slice_in_dim(weight_out, expert * FFW, FFW, 0)
        hidden = jnp.maximum(jnp.dot(block, first, preferred_element_type=jnp.float32), 0.0).astype(jnp.bfloat16)
        result = jnp.zeros((block_rows, width), jnp.float32)
        for piece in range(SLICES):
            partial_sum = jnp.dot(hidden[:, piece * FF_DEV:(piece + 1) * FF_DEV], second[piece * FF_DEV:(piece + 1) * FF_DEV, :], preferred_element_type=jnp.float32)
            rounded = lax.optimization_barrier(partial_sum.astype(jnp.bfloat16))
            result = result + rounded.astype(jnp.float32)
        valid = jnp.arange(block_rows, dtype=jnp.int32) < counts[expert]
        previous = lax.dynamic_slice_in_dim(results, start, block_rows, 0)
        merged = jnp.where(valid[:, None], result, previous)
        return lax.dynamic_update_slice_in_dim(results, merged, start, 0), 0

    initial = jnp.zeros((total_rows + block_rows, width), jnp.float32)
    results, unused = lax.scan(serve, initial, jnp.arange(EXPERTS, dtype=jnp.int32))
    expert_out = jnp.zeros((total_rows, width), jnp.float32).at[order].set(results[:total_rows])
    return (gates[:, None] * expert_out).astype(jnp.bfloat16)
```

```python
import functools

import jax
import jax.numpy as jnp
from jax import lax
from jax.experimental import pallas as pl
from jax.experimental.pallas import tpu as pltpu
from jax.sharding import PartitionSpec as P

SLICES = 4
CHUNKS = 4
BF16 = jnp.bfloat16
F32 = jnp.float32
MESH = pl.DeviceIdType.MESH


def layout(owner_count, tok_rows):
    groups = owner_count // SLICES
    chunks = min(CHUNKS, groups)
    per = groups // chunks
    seats = 3 * tok_rows // (4 * groups) + tok_rows // (2 * groups)
    unit = 8 if per == 1 else 16
    seats = -(-seats // unit) * unit
    offsets = [0]
    for far in range(1, groups // 2 + 1):
        offsets += [far, groups - far]
    return groups, chunks, per, seats, offsets[:groups]


def stack_rows(blocks):
    return jnp.concatenate([block.astype(F32) for block in blocks], axis=0).astype(BF16)


def kernel(
    owner_count,
    ids_col,
    ids_row,
    gates,
    tokens,
    weight_in,
    weight_out,
    out,
    w_in,
    w_out,
    send,
    gathered,
    staged,
    hidden,
    parts,
    diag_a,
    diag_b,
    from_x,
    from_y,
    sums,
    returned,
    w_sem,
    local_sem,
    z_send,
    z_recv,
    g_send,
    g_recv,
    r_send,
    r_recv,
    b_send,
    b_recv,
):
    tok_rows, width = tokens.shape
    groups, chunks, per, seats, offsets = layout(owner_count, tok_rows)
    half = width // 2
    me = lax.axis_index("ep")
    group = me // SLICES
    lane = me % SLICES
    x_bit, y_bit = lane % 2, lane // 2
    x_lane = y_bit * 2 + (1 - x_bit)
    y_lane = (1 - y_bit) * 2 + x_bit
    d_lane = (1 - y_bit) * 2 + (1 - x_bit)
    x_dev = group * SLICES + x_lane
    y_dev = group * SLICES + y_lane

    load_in = pltpu.make_async_copy(weight_in, w_in, w_sem.at[0])
    load_out = pltpu.make_async_copy(weight_out, w_out, w_sem.at[1])
    load_in.start()
    load_out.start()

    barrier = pltpu.get_barrier_semaphore()
    pl.semaphore_signal(barrier, inc=1, device_id={"ep": x_dev}, device_id_type=MESH)
    pl.semaphore_signal(barrier, inc=1, device_id={"ep": y_dev}, device_id_type=MESH)
    for off in range(1, groups):
        other = (group + off) % groups * SLICES + lane
        pl.semaphore_signal(barrier, inc=1, device_id={"ep": other}, device_id_type=MESH)

    slots = groups * seats
    lanes_e = -(-groups // 16) * 16
    t0 = lax.broadcasted_iota(jnp.int32, (tok_rows, tok_rows), 0)
    t1 = lax.broadcasted_iota(jnp.int32, (tok_rows, tok_rows), 1)
    ids_r = ids_row[...]
    hot_r = (lax.broadcasted_iota(jnp.int32, (lanes_e, tok_rows), 0) == ids_r).astype(F32)
    cum_r = jnp.dot(hot_r.astype(BF16), (t0 < t1).astype(F32).astype(BF16), preferred_element_type=F32)
    rank_r = jnp.sum(hot_r * cum_r, axis=0, keepdims=True).astype(jnp.int32)
    slot_r = ids_r * seats + rank_r
    place = (
        (lax.broadcasted_iota(jnp.int32, (slots, tok_rows), 0) == slot_r).astype(F32).astype(BF16)
    )
    step = 512
    for c in range(0, width, step):
        rows = jnp.dot(place, tokens[:, c : c + step], preferred_element_type=F32)
        for g in range(groups):
            send[g, :, c : c + step] = rows[g * seats : (g + 1) * seats].astype(BF16)

    pl.semaphore_wait(barrier, 2 + groups - 1)

    def remote(src, dst, s_sem, r_sem, dev):
        return pltpu.make_async_remote_copy(
            src_ref=src,
            dst_ref=dst,
            send_sem=s_sem,
            recv_sem=r_sem,
            device_id={"ep": dev},
            device_id_type=MESH,
        )

    def seat_block(ref, k):
        return ref.at[pl.ds(k % per * seats, seats)] if per > 1 else ref

    z_copies, local = {}, None
    for k in range(groups):
        target = (group - offsets[k] + groups) % groups
        dst = seat_block(gathered.at[k // per, lane], k)
        if k == 0:
            local = pltpu.make_async_copy(send.at[target], dst, local_sem.at[0])
            local.start()
        else:
            z_copies[k] = remote(
                send.at[target], dst, z_send.at[k], z_recv.at[k], target * SLICES + lane
            )
            z_copies[k].start()

    pending = list(z_copies.values())
    spread, forward, diag, pair, back = {}, {}, {}, {}, {}

    def stage_a(j):
        for k in range(j * per, (j + 1) * per):
            if k == 0:
                local.wait()
            else:
                z_copies[k].wait_recv()
        own = gathered.at[j, lane]
        spread[j] = [
            remote(own, own, g_send.at[j, 0], g_recv.at[j, 0], x_dev),
            remote(own, own, g_send.at[j, 1], g_recv.at[j, 1], y_dev),
        ]
        for copy in spread[j]:
            copy.start()

    def stage_b(j):
        first = gathered.at[j, x_lane, :, pl.ds(0, half)]
        second = gathered.at[j, y_lane, :, pl.ds(half, half)]
        forward[j] = [
            remote(first, first, g_send.at[j, 2], g_recv.at[j, 2], y_dev),
            remote(second, second, g_send.at[j, 3], g_recv.at[j, 3], x_dev),
        ]
        for arrived, onward in zip(spread[j], forward[j]):
            arrived.wait_recv()
            onward.start()

    def stage_c(j):
        for copy in forward[j]:
            copy.wait_recv()
        staged[...] = stack_rows([gathered[j, s] for s in range(SLICES)])
        if j == 0:
            load_in.wait()
        tile = 256
        rows = staged.shape[0] // SLICES

        @pl.loop(0, w_in.shape[1] // tile)
        def _(n):
            cols = pl.ds(pl.multiple_of(n * tile, tile), tile)
            value = jnp.dot(staged[...], w_in[:, cols], preferred_element_type=F32)
            hidden[:, cols] = jnp.maximum(value, 0.0).astype(BF16)

        if j == 0:
            load_out.wait()

        @pl.loop(0, width // tile)
        def _(n):
            cols = pl.ds(pl.multiple_of(n * tile, tile), tile)
            value = jnp.dot(hidden[...], w_out[:, cols], preferred_element_type=F32)
            for s in range(SLICES):
                parts[j, s, :, cols] = value[s * rows : (s + 1) * rows].astype(BF16)

    def stage_d(j):
        diag[j] = [
            remote(
                parts.at[j, d_lane, :, pl.ds(0, half)],
                diag_a.at[j],
                r_send.at[j, 0],
                r_recv.at[j, 0],
                y_dev,
            ),
            remote(
                parts.at[j, d_lane, :, pl.ds(half, half)],
                diag_b.at[j],
                r_send.at[j, 1],
                r_recv.at[j, 1],
                x_dev,
            ),
        ]
        for copy in diag[j]:
            copy.start()

    def stage_e(j):
        pair[j] = [
            remote(parts.at[j, x_lane], from_x.at[j], r_send.at[j, 2], r_recv.at[j, 2], x_dev),
            remote(parts.at[j, y_lane], from_y.at[j], r_send.at[j, 3], r_recv.at[j, 3], y_dev),
        ]
        diag[j][0].wait_recv()
        parts[j, x_lane, :, :half] = (
            parts[j, x_lane, :, :half].astype(F32) + diag_a[j].astype(F32)
        ).astype(BF16)
        diag[j][1].wait_recv()
        parts[j, y_lane, :, half:] = (
            parts[j, y_lane, :, half:].astype(F32) + diag_b[j].astype(F32)
        ).astype(BF16)
        for copy in pair[j]:
            copy.start()

    def stage_f(j):
        for copy in pair[j]:
            copy.wait_recv()
        sums[j] = (
            parts[j, lane].astype(F32) + from_x[j].astype(F32) + from_y[j].astype(F32)
        ).astype(BF16)
        for k in range(j * per, (j + 1) * per):
            source = (group + offsets[k]) % groups
            src = seat_block(sums.at[j], k)
            if k == 0:
                back[k] = pltpu.make_async_copy(src, returned.at[group], local_sem.at[1])
            else:
                back[k] = remote(
                    src, returned.at[group], b_send.at[k], b_recv.at[k], source * SLICES + lane
                )
            back[k].start()

    stages = [stage_a, stage_b, stage_c, stage_d, stage_e, stage_f]
    delay = [0, 1, 2, 2, 3, 4]
    for turn in range(chunks + max(delay)):
        for s in (0, 1, 4, 5, 2, 3):
            j = turn - delay[s]
            if 0 <= j < chunks:
                stages[s](j)

    ids_c = ids_col[...]
    hot_c = (lax.broadcasted_iota(jnp.int32, (tok_rows, 128), 1) == ids_c).astype(F32)
    cum_c = jnp.dot((t1 < t0).astype(F32).astype(BF16), hot_c.astype(BF16), preferred_element_type=F32)
    rank_c = jnp.sum(hot_c * cum_c, axis=1, keepdims=True).astype(jnp.int32)
    slot_c = ids_c * seats + rank_c
    pick = (
        (lax.broadcasted_iota(jnp.int32, (tok_rows, slots), 1) == slot_c).astype(F32).astype(BF16)
    )
    weight = gates[...]
    for k in range(groups):
        if k == 0:
            back[k].wait()
        else:
            back[k].wait_recv()
    for c in range(0, width, step):
        block = stack_rows([returned[g, :, c : c + step] for g in range(groups)])
        picked = jnp.dot(pick, block, preferred_element_type=F32)
        out[:, c : c + step] = (weight * picked).astype(BF16)

    for j in range(chunks):
        for copy in spread[j] + forward[j] + diag[j] + pair[j]:
            copy.wait_send()
    for k in range(1, groups):
        z_copies[k].wait_send()
        back[k].wait_send()


def body(tokens, gates, expert_ids, weight_in, weight_out):
    owner_count = lax.axis_size("ep")
    tok_rows, width = tokens.shape
    groups, chunks, per, seats, _ = layout(owner_count, tok_rows)
    rows = per * seats
    half = width // 2
    vmem = pl.BlockSpec(memory_space=pltpu.VMEM)
    hbm = pl.BlockSpec(memory_space=pl.ANY)
    dma = pltpu.SemaphoreType.DMA
    return pl.pallas_call(
        functools.partial(kernel, owner_count),
        out_shape=jax.ShapeDtypeStruct((tok_rows, width), BF16),
        in_specs=[vmem] * 4 + [hbm] * 2,
        out_specs=vmem,
        scratch_shapes=[
            pltpu.VMEM(weight_in.shape, BF16),
            pltpu.VMEM(weight_out.shape, BF16),
            pltpu.VMEM((groups, seats, width), BF16),
            pltpu.VMEM((chunks, SLICES, rows, width), BF16),
            pltpu.VMEM((SLICES * rows, width), BF16),
            pltpu.VMEM((SLICES * rows, weight_in.shape[1]), BF16),
            pltpu.VMEM((chunks, SLICES, rows, width), BF16),
            pltpu.VMEM((chunks, rows, half), BF16),
            pltpu.VMEM((chunks, rows, half), BF16),
            pltpu.VMEM((chunks, rows, width), BF16),
            pltpu.VMEM((chunks, rows, width), BF16),
            pltpu.VMEM((chunks, rows, width), BF16),
            pltpu.VMEM((groups, seats, width), BF16),
            dma((2,)),
            dma((2,)),
            dma((groups,)),
            dma((groups,)),
            dma((chunks, 4)),
            dma((chunks, 4)),
            dma((chunks, 4)),
            dma((chunks, 4)),
            dma((groups,)),
            dma((groups,)),
        ],
        compiler_params=pltpu.CompilerParams(
            collective_id=0, has_side_effects=True, vmem_limit_bytes=60 * 1024 * 1024
        ),
    )(
        expert_ids,
        expert_ids.reshape(1, tok_rows),
        gates.reshape(tok_rows, 1),
        tokens,
        weight_in,
        weight_out,
    )


def solution(mesh):
    in_specs = (
        P(("rep", "ep"), None),
        P(("rep", "ep")),
        P(("rep", "ep"), None),
        P(None, "ep"),
        P("ep", None),
    )
    out_specs = P(("rep", "ep"), None)
    return jax.shard_map(body, mesh=mesh, in_specs=in_specs, out_specs=out_specs, check_vma=False)
```

```python
import functools

import jax
import jax.numpy as jnp
from jax import lax
from jax.experimental import pallas as pl
from jax.experimental.pallas import tpu as pltpu
from jax.sharding import PartitionSpec as P

SLICES = 4
CHUNKS = 4
STEP = 512
ORDER = "a1b0a2b1c0a3b2c1d1b3c2d2e1c3d3e2d0f1e3f2e0f3f0"
BF16 = jnp.bfloat16
F32 = jnp.float32
MESH = pl.DeviceIdType.MESH


def layout(owner_count, tok_rows):
    groups = owner_count // SLICES
    chunks = CHUNKS
    per = groups // chunks
    seats = 3 * tok_rows // (4 * groups) + tok_rows // (2 * groups)
    unit = 8 if per == 1 else 16
    seats = -(-seats // unit) * unit
    offsets = [0]
    for far in range(1, groups // 2 + 1):
        offsets += [far, groups - far]
    return groups, chunks, per, seats, offsets[:groups]


def stack_rows(blocks):
    return jnp.concatenate([block.astype(F32) for block in blocks], axis=0).astype(BF16)


def kernel(
    owner_count,
    ids_row,
    gates,
    tokens,
    weight_in,
    weight_out,
    out,
    w_in,
    w_out,
    send,
    gathered,
    staged,
    hidden,
    parts,
    diag_a,
    diag_b,
    from_x,
    from_y,
    sums,
    returned,
    w_sem,
    z_send,
    z_recv,
    g_send,
    g_recv,
    r_send,
    r_recv,
    b_send,
    b_recv,
):
    tok_rows, width = tokens.shape
    groups, chunks, per, seats, offsets = layout(owner_count, tok_rows)
    half = width // 2
    me = lax.axis_index("ep")
    group = me // SLICES
    lane = me % SLICES
    x_bit, y_bit = lane % 2, lane // 2
    x_lane = y_bit * 2 + (1 - x_bit)
    y_lane = (1 - y_bit) * 2 + x_bit
    d_lane = (1 - y_bit) * 2 + (1 - x_bit)
    x_dev = group * SLICES + x_lane
    y_dev = group * SLICES + y_lane

    load_in = pltpu.make_async_copy(weight_in, w_in, w_sem.at[0])
    load_out = pltpu.make_async_copy(weight_out, w_out, w_sem.at[1])
    load_in.start()
    load_out.start()

    barrier = pltpu.get_barrier_semaphore()
    pl.semaphore_signal(barrier, inc=1, device_id={"ep": x_dev}, device_id_type=MESH)
    pl.semaphore_signal(barrier, inc=1, device_id={"ep": y_dev}, device_id_type=MESH)
    for off in range(1, groups):
        other = (group + off) % groups * SLICES + lane
        pl.semaphore_signal(barrier, inc=1, device_id={"ep": other}, device_id_type=MESH)

    lanes_e = -(-groups // 16) * 16
    t0 = lax.broadcasted_iota(jnp.int32, (tok_rows, tok_rows), 0)
    t1 = lax.broadcasted_iota(jnp.int32, (tok_rows, tok_rows), 1)
    ids = ids_row[...]
    hot = (lax.broadcasted_iota(jnp.int32, (lanes_e, tok_rows), 0) == ids).astype(F32)
    ahead = jnp.dot(hot.astype(BF16), (t0 < t1).astype(F32).astype(BF16), preferred_element_type=F32)
    slot = ids * seats + jnp.sum(hot * ahead, axis=0, keepdims=True).astype(jnp.int32)

    def take(target, dst):
        seat = lax.broadcasted_iota(jnp.int32, (seats, tok_rows), 0) + target * seats
        place = (seat == slot).astype(F32).astype(BF16)
        for c in range(0, width, STEP):
            rows = jnp.dot(place, tokens[:, c : c + STEP], preferred_element_type=F32)
            dst[:, c : c + STEP] = rows.astype(BF16)

    def remote(src, dst, s_sem, r_sem, dev):
        return pltpu.make_async_remote_copy(
            src_ref=src,
            dst_ref=dst,
            send_sem=s_sem,
            recv_sem=r_sem,
            device_id={"ep": dev},
            device_id_type=MESH,
        )

    def seat_block(ref, k):
        return ref.at[pl.ds(k % per * seats, seats)] if per > 1 else ref

    spread, forward, diag, pair, z_copies, back = {}, {}, {}, {}, {}, {}

    def take_for(k):
        target = (group - offsets[k] + groups) % groups
        take(target, send.at[k])
        z_copies[k] = remote(
            send.at[k],
            seat_block(gathered.at[k // per, lane], k),
            z_send.at[k],
            z_recv.at[k],
            target * SLICES + lane,
        )

    def stage_a(j):
        for k in range(j * per, (j + 1) * per):
            if k > 0:
                z_copies[k].wait_recv()
        own = gathered.at[j, lane]
        spread[j] = [
            remote(own, own, g_send.at[j, 0], g_recv.at[j, 0], x_dev),
            remote(own, own, g_send.at[j, 1], g_recv.at[j, 1], y_dev),
        ]
        for copy in spread[j]:
            copy.start()

    def stage_b(j):
        first = gathered.at[j, x_lane, :, pl.ds(0, half)]
        second = gathered.at[j, y_lane, :, pl.ds(half, half)]
        forward[j] = [
            remote(first, first, g_send.at[j, 2], g_recv.at[j, 2], y_dev),
            remote(second, second, g_send.at[j, 3], g_recv.at[j, 3], x_dev),
        ]
        for arrived, onward in zip(spread[j], forward[j]):
            arrived.wait_recv()
            onward.start()

    def stage_c(j):
        for copy in forward[j]:
            copy.wait_recv()
        staged[...] = stack_rows([gathered[j, s] for s in range(SLICES)])
        if j == 0:
            load_in.wait()
        tile = STEP
        rows = staged.shape[0] // SLICES

        @pl.loop(0, w_in.shape[1] // tile)
        def _(n):
            cols = pl.ds(pl.multiple_of(n * tile, tile), tile)
            value = jnp.dot(staged[...], w_in[:, cols], preferred_element_type=F32)
            hidden[:, cols] = jnp.maximum(value, 0.0).astype(BF16)

        if j == 0:
            load_out.wait()

        @pl.loop(0, width // tile)
        def _(n):
            cols = pl.ds(pl.multiple_of(n * tile, tile), tile)
            value = jnp.dot(hidden[...], w_out[:, cols], preferred_element_type=F32)
            for s in range(SLICES):
                parts[j, s, :, cols] = value[s * rows : (s + 1) * rows].astype(BF16)

    def stage_d(j):
        diag[j] = [
            remote(
                parts.at[j, d_lane, :, pl.ds(0, half)],
                diag_a.at[j],
                r_send.at[j, 0],
                r_recv.at[j, 0],
                y_dev,
            ),
            remote(
                parts.at[j, d_lane, :, pl.ds(half, half)],
                diag_b.at[j],
                r_send.at[j, 1],
                r_recv.at[j, 1],
                x_dev,
            ),
        ]
        for copy in diag[j]:
            copy.start()

    def stage_e(j):
        pair[j] = [
            remote(parts.at[j, x_lane], from_x.at[j], r_send.at[j, 2], r_recv.at[j, 2], x_dev),
            remote(parts.at[j, y_lane], from_y.at[j], r_send.at[j, 3], r_recv.at[j, 3], y_dev),
        ]
        diag[j][0].wait_recv()
        parts[j, x_lane, :, :half] = (
            parts[j, x_lane, :, :half].astype(F32) + diag_a[j].astype(F32)
        ).astype(BF16)
        diag[j][1].wait_recv()
        parts[j, y_lane, :, half:] = (
            parts[j, y_lane, :, half:].astype(F32) + diag_b[j].astype(F32)
        ).astype(BF16)
        for copy in pair[j]:
            copy.start()

    def stage_f(j):
        for copy in pair[j]:
            copy.wait_recv()
        sums[j] = (
            parts[j, lane].astype(F32) + from_x[j].astype(F32) + from_y[j].astype(F32)
        ).astype(BF16)
        for k in range(j * per, (j + 1) * per):
            if k > 0:
                source = (group + offsets[k]) % groups
                src = seat_block(sums.at[j], k)
                back[k] = remote(
                    src, returned.at[k], b_send.at[k], b_recv.at[k], source * SLICES + lane
                )
                back[k].start()

    take(group, seat_block(gathered.at[0, lane], 0))
    take_for(1)
    pl.semaphore_wait(barrier, 2 + groups - 1)
    if per == 1:
        stage_a(0)
    for k in range(2, groups):
        take_for(k)
        z_copies[k - 1].start()
    z_copies[groups - 1].start()
    if per > 1:
        stage_a(0)

    stages = {"a": stage_a, "b": stage_b, "c": stage_c, "d": stage_d, "e": stage_e, "f": stage_f}
    for name, j in zip(ORDER[::2], ORDER[1::2]):
        stages[name](int(j))

    slot_c = jnp.sum(jnp.where(t0 == t1, slot, 0), axis=1, keepdims=True)
    weight = jnp.sum(jnp.where(t0 == t1, gates[...], 0.0), axis=1, keepdims=True)
    picks = []
    for k in range(groups):
        if k > 0:
            back[k].wait_recv()
        target = (group - offsets[k] + groups) % groups
        seat = lax.broadcasted_iota(jnp.int32, (tok_rows, seats), 1) + target * seats
        picks.append((seat == slot_c).astype(F32))
    pick = jnp.concatenate(picks, axis=1).astype(BF16)
    for c in range(0, width, STEP):
        blocks = [sums[0, :seats, c : c + STEP]]
        blocks += [returned[k, :, c : c + STEP] for k in range(1, groups)]
        picked = jnp.dot(pick, stack_rows(blocks), preferred_element_type=F32)
        out[:, c : c + STEP] = (weight * picked).astype(BF16)

    for j in range(chunks):
        for copy in spread[j] + forward[j] + diag[j] + pair[j]:
            copy.wait_send()
    for k in range(1, groups):
        z_copies[k].wait_send()
        back[k].wait_send()


def body(tokens, gates, expert_ids, weight_in, weight_out):
    owner_count = lax.axis_size("ep")
    tok_rows, width = tokens.shape
    groups, chunks, per, seats, _ = layout(owner_count, tok_rows)
    rows = per * seats
    half = width // 2
    vmem = pl.BlockSpec(memory_space=pltpu.VMEM)
    hbm = pl.BlockSpec(memory_space=pl.ANY)
    dma = pltpu.SemaphoreType.DMA
    return pl.pallas_call(
        functools.partial(kernel, owner_count),
        out_shape=jax.ShapeDtypeStruct((tok_rows, width), BF16),
        in_specs=[vmem] * 3 + [hbm] * 2,
        out_specs=vmem,
        scratch_shapes=[
            pltpu.VMEM(weight_in.shape, BF16),
            pltpu.VMEM(weight_out.shape, BF16),
            pltpu.VMEM((groups, seats, width), BF16),
            pltpu.VMEM((chunks, SLICES, rows, width), BF16),
            pltpu.VMEM((SLICES * rows, width), BF16),
            pltpu.VMEM((SLICES * rows, weight_in.shape[1]), BF16),
            pltpu.VMEM((chunks, SLICES, rows, width), BF16),
            pltpu.VMEM((chunks, rows, half), BF16),
            pltpu.VMEM((chunks, rows, half), BF16),
            pltpu.VMEM((chunks, rows, width), BF16),
            pltpu.VMEM((chunks, rows, width), BF16),
            pltpu.VMEM((chunks, rows, width), BF16),
            pltpu.VMEM((groups, seats, width), BF16),
            dma((2,)),
            dma((groups,)),
            dma((groups,)),
            dma((chunks, 4)),
            dma((chunks, 4)),
            dma((chunks, 4)),
            dma((chunks, 4)),
            dma((groups,)),
            dma((groups,)),
        ],
        compiler_params=pltpu.CompilerParams(
            collective_id=0, has_side_effects=True, vmem_limit_bytes=60 * 1024 * 1024
        ),
    )(
        expert_ids.reshape(1, tok_rows),
        gates.reshape(1, tok_rows),
        tokens,
        weight_in,
        weight_out,
    )


def solution(mesh):
    in_specs = (
        P(("rep", "ep"), None),
        P(("rep", "ep")),
        P(("rep", "ep"), None),
        P(None, "ep"),
        P("ep", None),
    )
    out_specs = P(("rep", "ep"), None)
    return jax.shard_map(body, mesh=mesh, in_specs=in_specs, out_specs=out_specs, check_vma=False)
```

```python
import functools

import jax
import jax.numpy as jnp
from jax import lax
from jax.experimental import pallas as pl
from jax.experimental.pallas import tpu as pltpu
from jax.sharding import PartitionSpec as P

SLICES = 4
CHUNKS = 4
STEP = 512
ORDER = "a1b0a2b1c0a3b2c1d1b3c2d2e1c3d3e2d0f1e3f2e0f3f0"
BF16 = jnp.bfloat16
F32 = jnp.float32
MESH = pl.DeviceIdType.MESH


def layout(owner_count, tok_rows):
    groups = owner_count // SLICES
    chunks = CHUNKS
    per = groups // chunks
    seats = 3 * tok_rows // (4 * groups) + tok_rows // (2 * groups)
    unit = 8 if per == 1 else 16
    seats = -(-seats // unit) * unit
    offsets = [0]
    for far in range(1, groups // 2 + 1):
        offsets += [far, groups - far]
    return groups, chunks, per, seats, offsets[:groups]


def stack_rows(blocks):
    return jnp.concatenate([block.astype(F32) for block in blocks], axis=0).astype(BF16)


def kernel(
    owner_count,
    ids_row,
    gates,
    tokens,
    weight_in,
    weight_out,
    out,
    w_in,
    w_out,
    send,
    gathered,
    staged,
    hidden,
    parts,
    diag_a,
    diag_b,
    from_x,
    from_y,
    sums,
    returned,
    w_sem,
    z_send,
    z_recv,
    g_send,
    g_recv,
    r_send,
    r_recv,
    b_send,
    b_recv,
):
    tok_rows, width = tokens.shape
    groups, chunks, per, seats, offsets = layout(owner_count, tok_rows)
    half = width // 2
    me = lax.axis_index("ep")
    group = me // SLICES
    lane = me % SLICES
    x_bit, y_bit = lane % 2, lane // 2
    x_lane = y_bit * 2 + (1 - x_bit)
    y_lane = (1 - y_bit) * 2 + x_bit
    d_lane = (1 - y_bit) * 2 + (1 - x_bit)
    x_dev = group * SLICES + x_lane
    y_dev = group * SLICES + y_lane

    load_in = pltpu.make_async_copy(weight_in, w_in, w_sem.at[0])
    load_out = pltpu.make_async_copy(weight_out, w_out, w_sem.at[1])
    load_in.start()
    load_out.start()

    barrier = pltpu.get_barrier_semaphore()
    pl.semaphore_signal(barrier, inc=1, device_id={"ep": x_dev}, device_id_type=MESH)
    pl.semaphore_signal(barrier, inc=1, device_id={"ep": y_dev}, device_id_type=MESH)
    for off in range(1, groups):
        other = (group + off) % groups * SLICES + lane
        pl.semaphore_signal(barrier, inc=1, device_id={"ep": other}, device_id_type=MESH)

    lanes_e = -(-groups // 16) * 16
    t0 = lax.broadcasted_iota(jnp.int32, (tok_rows, tok_rows), 0)
    t1 = lax.broadcasted_iota(jnp.int32, (tok_rows, tok_rows), 1)
    ids = ids_row[...]
    hot = (lax.broadcasted_iota(jnp.int32, (lanes_e, tok_rows), 0) == ids).astype(F32)
    ahead = jnp.dot(hot.astype(BF16), (t0 < t1).astype(F32).astype(BF16), preferred_element_type=F32)
    slot = ids * seats + jnp.sum(hot * ahead, axis=0, keepdims=True).astype(jnp.int32)

    def take(target, dst):
        seat = lax.broadcasted_iota(jnp.int32, (seats, tok_rows), 0) + target * seats
        place = (seat == slot).astype(F32).astype(BF16)
        for c in range(0, width, STEP):
            rows = jnp.dot(place, tokens[:, c : c + STEP], preferred_element_type=F32)
            dst[:, c : c + STEP] = rows.astype(BF16)

    def remote(src, dst, s_sem, r_sem, dev):
        return pltpu.make_async_remote_copy(
            src_ref=src,
            dst_ref=dst,
            send_sem=s_sem,
            recv_sem=r_sem,
            device_id={"ep": dev},
            device_id_type=MESH,
        )

    def seat_block(ref, k):
        return ref.at[pl.ds(k % per * seats, seats)] if per > 1 else ref

    spread, forward, diag, pair, z_copies, back = {}, {}, {}, {}, {}, {}

    def take_for(k):
        target = (group - offsets[k] + groups) % groups
        take(target, send.at[k])
        z_copies[k] = remote(
            send.at[k],
            seat_block(gathered.at[k // per, lane], k),
            z_send.at[k],
            z_recv.at[k],
            target * SLICES + lane,
        )

    def stage_a(j):
        for k in range(j * per, (j + 1) * per):
            if k > 0:
                z_copies[k].wait_recv()
        own = gathered.at[j, lane]
        spread[j] = [
            remote(own, own, g_send.at[j, 0], g_recv.at[j, 0], x_dev),
            remote(own, own, g_send.at[j, 1], g_recv.at[j, 1], y_dev),
        ]
        for copy in spread[j]:
            copy.start()

    def stage_b(j):
        first = gathered.at[j, x_lane, :, pl.ds(0, half)]
        second = gathered.at[j, y_lane, :, pl.ds(half, half)]
        forward[j] = [
            remote(first, first, g_send.at[j, 2], g_recv.at[j, 2], y_dev),
            remote(second, second, g_send.at[j, 3], g_recv.at[j, 3], x_dev),
        ]
        for arrived, onward in zip(spread[j], forward[j]):
            arrived.wait_recv()
            onward.start()

    def stage_c(j):
        for copy in forward[j]:
            copy.wait_recv()
        staged[...] = stack_rows([gathered[j, s] for s in range(SLICES)])
        if j == 0:
            load_in.wait()
        tile = STEP
        rows = staged.shape[0] // SLICES

        @pl.loop(0, w_in.shape[1] // tile)
        def _(n):
            cols = pl.ds(pl.multiple_of(n * tile, tile), tile)
            value = jnp.dot(staged[...], w_in[:, cols], preferred_element_type=F32)
            hidden[:, cols] = jnp.maximum(value, 0.0).astype(BF16)

        if j == 0:
            load_out.wait()

        @pl.loop(0, width // tile)
        def _(n):
            cols = pl.ds(pl.multiple_of(n * tile, tile), tile)
            value = jnp.dot(hidden[...], w_out[:, cols], preferred_element_type=F32)
            for s in range(SLICES):
                parts[j, s, :, cols] = value[s * rows : (s + 1) * rows].astype(BF16)

    def stage_d(j):
        diag[j] = [
            remote(
                parts.at[j, d_lane, :, pl.ds(0, half)],
                diag_a.at[j],
                r_send.at[j, 0],
                r_recv.at[j, 0],
                y_dev,
            ),
            remote(
                parts.at[j, d_lane, :, pl.ds(half, half)],
                diag_b.at[j],
                r_send.at[j, 1],
                r_recv.at[j, 1],
                x_dev,
            ),
        ]
        for copy in diag[j]:
            copy.start()

    def stage_e(j):
        pair[j] = [
            remote(parts.at[j, x_lane], from_x.at[j], r_send.at[j, 2], r_recv.at[j, 2], x_dev),
            remote(parts.at[j, y_lane], from_y.at[j], r_send.at[j, 3], r_recv.at[j, 3], y_dev),
        ]
        diag[j][0].wait_recv()
        parts[j, x_lane, :, :half] = (
            parts[j, x_lane, :, :half].astype(F32) + diag_a[j].astype(F32)
        ).astype(BF16)
        pair[j][0].start()
        diag[j][1].wait_recv()
        parts[j, y_lane, :, half:] = (
            parts[j, y_lane, :, half:].astype(F32) + diag_b[j].astype(F32)
        ).astype(BF16)
        pair[j][1].start()

    def stage_f(j):
        for copy in pair[j]:
            copy.wait_recv()
        sums[j] = (
            parts[j, lane].astype(F32) + from_x[j].astype(F32) + from_y[j].astype(F32)
        ).astype(BF16)
        for k in range(j * per, (j + 1) * per):
            if k > 0:
                source = (group + offsets[k]) % groups
                src = seat_block(sums.at[j], k)
                back[k] = remote(
                    src, returned.at[k], b_send.at[k], b_recv.at[k], source * SLICES + lane
                )
                back[k].start()

    take(group, seat_block(gathered.at[0, lane], 0))
    take_for(1)
    pl.semaphore_wait(barrier, 2 + groups - 1)
    if per == 1:
        stage_a(0)
    for k in range(2, groups):
        take_for(k)
        z_copies[k - 1].start()
    z_copies[groups - 1].start()
    if per > 1:
        stage_a(0)

    stages = {"a": stage_a, "b": stage_b, "c": stage_c, "d": stage_d, "e": stage_e, "f": stage_f}
    for name, j in zip(ORDER[::2], ORDER[1::2]):
        stages[name](int(j))

    slot_c = jnp.sum(jnp.where(t0 == t1, slot, 0), axis=1, keepdims=True)
    weight = jnp.sum(jnp.where(t0 == t1, gates[...], 0.0), axis=1, keepdims=True)
    picks = []
    for k in range(groups):
        if k > 0:
            back[k].wait_recv()
        target = (group - offsets[k] + groups) % groups
        seat = lax.broadcasted_iota(jnp.int32, (tok_rows, seats), 1) + target * seats
        picks.append((seat == slot_c).astype(F32))
    pick = jnp.concatenate(picks, axis=1).astype(BF16)
    for c in range(0, width, STEP):
        blocks = [sums[0, :seats, c : c + STEP]]
        blocks += [returned[k, :, c : c + STEP] for k in range(1, groups)]
        picked = jnp.dot(pick, stack_rows(blocks), preferred_element_type=F32)
        out[:, c : c + STEP] = (weight * picked).astype(BF16)

    for j in range(chunks):
        for copy in spread[j] + forward[j] + diag[j] + pair[j]:
            copy.wait_send()
    for k in range(1, groups):
        z_copies[k].wait_send()
        back[k].wait_send()


def body(tokens, gates, expert_ids, weight_in, weight_out):
    owner_count = lax.axis_size("ep")
    tok_rows, width = tokens.shape
    groups, chunks, per, seats, _ = layout(owner_count, tok_rows)
    rows = per * seats
    half = width // 2
    vmem = pl.BlockSpec(memory_space=pltpu.VMEM)
    hbm = pl.BlockSpec(memory_space=pl.ANY)
    dma = pltpu.SemaphoreType.DMA
    return pl.pallas_call(
        functools.partial(kernel, owner_count),
        out_shape=jax.ShapeDtypeStruct((tok_rows, width), BF16),
        in_specs=[vmem] * 3 + [hbm] * 2,
        out_specs=vmem,
        scratch_shapes=[
            pltpu.VMEM(weight_in.shape, BF16),
            pltpu.VMEM(weight_out.shape, BF16),
            pltpu.VMEM((groups, seats, width), BF16),
            pltpu.VMEM((chunks, SLICES, rows, width), BF16),
            pltpu.VMEM((SLICES * rows, width), BF16),
            pltpu.VMEM((SLICES * rows, weight_in.shape[1]), BF16),
            pltpu.VMEM((chunks, SLICES, rows, width), BF16),
            pltpu.VMEM((chunks, rows, half), BF16),
            pltpu.VMEM((chunks, rows, half), BF16),
            pltpu.VMEM((chunks, rows, width), BF16),
            pltpu.VMEM((chunks, rows, width), BF16),
            pltpu.VMEM((chunks, rows, width), BF16),
            pltpu.VMEM((groups, seats, width), BF16),
            dma((2,)),
            dma((groups,)),
            dma((groups,)),
            dma((chunks, 4)),
            dma((chunks, 4)),
            dma((chunks, 4)),
            dma((chunks, 4)),
            dma((groups,)),
            dma((groups,)),
        ],
        compiler_params=pltpu.CompilerParams(
            collective_id=0, has_side_effects=True, vmem_limit_bytes=60 * 1024 * 1024
        ),
    )(
        expert_ids.reshape(1, tok_rows),
        gates.reshape(1, tok_rows),
        tokens,
        weight_in,
        weight_out,
    )


def solution(mesh):
    in_specs = (
        P(("rep", "ep"), None),
        P(("rep", "ep")),
        P(("rep", "ep"), None),
        P(None, "ep"),
        P("ep", None),
    )
    out_specs = P(("rep", "ep"), None)
    return jax.shard_map(body, mesh=mesh, in_specs=in_specs, out_specs=out_specs, check_vma=False)
```
